32 devices in a mesh: data: 4 (over x, y), expert: 8 (over z, core).
Axes of the slice: x: 2, y: 2, z: 4, core: 2. Of those that a mesh axis runs over, the one named last changes fastest.
Arguments:
- x: bfloat16 [32768, 2048], P(('data', 'expert')), parts along dimension 0
- idx: int32 [32768, 2], P(('data', 'expert')), parts along dimension 0
- wr: bfloat16 [2048, 8], replicated
- w1: bfloat16 [8, 2048, 5632], P('expert')
- w3: bfloat16 [8, 2048, 5632], P('expert')
- w2: bfloat16 [8, 5632, 2048], P('expert')
Outputs:
- output: bfloat16 [32768, 2048], P(('data', 'expert')), parts along dimension 0
There are 4 independent parts. The reference program is written for one: setup_inputs(seed, part) draws one part's arguments, and reference() takes and returns one part's arrays. A program takes and returns all parts, laid end to end along the dimension named above; an argument that names none is the same for every part.
All inputs are finite; a program needn't handle non-finite values.
Results may differ from the reference program's by a relative error of at most 0.00141.
Values are sent between devices in bfloat16 or wider.
A program may use at most 1 GiB of HBM per device.

```python
import jax
import jax.numpy as jnp
from jax import lax

N = 8
T = 1024
D = 2048
FF = 5632
TOP = 2
E = 8
CS = 512


def _routing(key):
    h = E // 2

    def one(k):
        kh, kp, ks = jax.random.split(k, 3)
        hot = jax.random.permutation(kh, E)[:h]
        p = jax.random.permutation(kp, T)
        e0 = hot[p % h]
        e1 = (e0 + 1 + (p // h) % (E - 1)) % E
        pair = jnp.stack([e0, e1], axis=1)
        swap = jax.random.bernoulli(ks, 0.5, (T, 1))
        return jnp.where(swap, pair[:, ::-1], pair)
    return jax.vmap(one)(jax.random.split(key, N)).reshape(N * T, TOP).astype(jnp.int32)


def setup_inputs(seed: int = 0, part: int = 0) -> dict:
    key = jax.random.key(seed)
    kshared, kpart = jax.random.split(key)
    kx, ki = jax.random.split(jax.random.fold_in(kpart, part))
    kr, k1, k3, k2 = jax.random.split(kshared, 4)
    x = jax.random.normal(kx, (N * T, D), jnp.float32).astype(jnp.bfloat16)
    wr = (jax.random.normal(kr, (D, E), jnp.float32) * (1.5 * D ** -0.5)).astype(jnp.bfloat16)
    w1 = (jax.random.normal(k1, (E, D, FF), jnp.float32) * D ** -0.5).astype(jnp.bfloat16)
    w3 = (jax.random.normal(k3, (E, D, FF), jnp.float32) * D ** -0.5).astype(jnp.bfloat16)
    w2 = (jax.random.normal(k2, (E, FF, D), jnp.float32) * FF ** -0.5).astype(jnp.bfloat16)
    return {'x': x, 'idx': _routing(jax.random.fold_in(ki, 7)), 'wr': wr, 'w1': w1, 'w3': w3, 'w2': w2}


def reference(x, idx, wr, w1, w3, w2):
    logits = jnp.dot(x, wr, preferred_element_type=jnp.float32)
    g = jax.nn.softmax(jnp.take_along_axis(logits, idx, axis=1), axis=-1)
    e = idx.reshape(N, T * TOP)
    oh = (e[:, :, None] == jnp.arange(E, dtype=jnp.int32)[None, None, :]).astype(jnp.int32)
    pos = jnp.take_along_axis(jnp.cumsum(oh, axis=1), e[:, :, None], axis=2)[:, :, 0] - 1
    src = jnp.arange(N, dtype=jnp.int32)[:, None]
    valid = (pos < CS).reshape(-1)
    dest = jnp.where(valid, ((e * N + src) * CS + pos).reshape(-1), E * N * CS)
    rows = jnp.repeat(x, TOP, axis=0)
    buf = jnp.zeros((E * N * CS, D), jnp.bfloat16).at[dest].set(rows, mode='drop').reshape(E, N * CS, D)

    def expert(args):
        xb, a1, a3, a2 = args
        h1 = jnp.dot(xb, a1, preferred_element_type=jnp.float32)
        h3 = jnp.dot(xb, a3, preferred_element_type=jnp.float32)
        h = (jax.nn.silu(h1) * h3).astype(jnp.bfloat16)
        return jnp.dot(h, a2, preferred_element_type=jnp.float32).astype(jnp.bfloat16)

    o = lax.map(expert, (buf, w1, w3, w2)).reshape(E * N * CS, D)
    op = jnp.where(valid[:, None], o[jnp.where(valid, dest, 0)], 0)
    y = jnp.sum(g[:, :, None] * op.reshape(N * T, TOP, D).astype(jnp.float32), axis=1)
    return y.astype(jnp.bfloat16)
```

```python
import functools

import jax
import jax.numpy as jnp
from jax import lax
from jax.experimental import pallas as pl
from jax.experimental.pallas import tpu as pltpu
from jax.sharding import PartitionSpec as P

MT = 256
FT = 512
DT = 512
PIECE = 16
FAST = (176, 192)
VMEM = 62 * 1024 * 1024


def _params():
    return pltpu.CompilerParams(vmem_limit_bytes=VMEM)


def _cost(flops, moved):
    return pl.CostEstimate(flops=flops, bytes_accessed=moved, transcendentals=0)


def _gather_kernel(base, n, dest_ref, x_ref, *refs):
    outs, buf, sem = refs[:n], refs[n], refs[n + 1]
    i = pl.program_id(0)
    rows, t = buf.shape[1], x_ref.shape[0]
    r = lax.broadcasted_iota(jnp.int32, (rows, t), 0) + (base + i * rows)
    hit = (r == dest_ref[0:1, :]) | (r == dest_ref[1:2, :])
    buf[i] = jnp.dot(hit.astype(jnp.bfloat16), x_ref[...], preferred_element_type=jnp.float32).astype(buf.dtype)
    for s in range(n):
        @pl.when(i == s)
        def _():
            pltpu.make_async_copy(buf.at[s], outs[s], sem.at[s]).start()

    @pl.when(i == n - 1)
    def _():
        for s in range(n):
            pltpu.make_async_copy(buf.at[s], outs[s], sem.at[s]).wait()


def _gather(x, dest_t, base, rows, n, name):
    t, d = x.shape
    return pl.pallas_call(
        functools.partial(_gather_kernel, base, n),
        grid=(n,),
        in_specs=[
            pl.BlockSpec((2, t), lambda i: (0, 0)),
            pl.BlockSpec((t, d), lambda i: (0, 0), pipeline_mode=pl.Buffered(1)),
        ],
        out_specs=[pl.BlockSpec(memory_space=pl.ANY)] * n,
        out_shape=[jax.ShapeDtypeStruct((rows, d), x.dtype)] * n,
        scratch_shapes=[pltpu.VMEM((n, rows, d), x.dtype), pltpu.SemaphoreType.DMA((n,))],
        compiler_params=_params(),
        cost_estimate=_cost(2 * n * rows * t * d, 2 * d * (t + n * rows)),
        name=name,
    )(dest_t, x)


def _mlp_kernel(nf, nd, n, off_ref, *refs):
    srcs, (w1_ref, w3_ref, w2_ref), outs = refs[:n], refs[n : n + 3], refs[n + 3 : 2 * n + 3]
    xs, hs, os, in_sem, out_sem = refs[2 * n + 3 :]
    i = pl.program_id(0)
    seg = srcs[0].shape[0]
    tiles = (off_ref[n] + (MT - 1)) // MT

    def place(s):
        return pl.ds(pl.multiple_of(off_ref[s], PIECE), seg)

    def put(s, j):
        return pltpu.make_async_copy(
            os.at[j % 2, place(s), :], outs[s].at[:, pl.ds(j * DT, DT)], out_sem.at[j % 2, s]
        )

    @pl.when(i == 0)
    def _():
        def clear(r, c):
            rows = pl.ds(pl.multiple_of(r * 128, 128), 128)
            xs[rows, :] = jnp.zeros((128, xs.shape[1]), xs.dtype)
            for b in range(2):
                os[b, rows, :] = jnp.zeros((128, DT), os.dtype)
            return c

        lax.fori_loop(0, xs.shape[0] // 128, clear, 0)

        def piece(s, p):
            at = pl.multiple_of(off_ref[s] + p * PIECE, PIECE)
            src = srcs[s].at[pl.ds(pl.multiple_of(p * PIECE, PIECE), PIECE), :]
            return pltpu.make_async_copy(src, xs.at[pl.ds(at, PIECE), :], in_sem.at[s, p])

        def each(s, act):
            def body(p, c):
                act(piece(s, p))
                return c

            lax.fori_loop(0, (off_ref[s + 1] - off_ref[s]) // PIECE, body, 0)

        for s in range(n):
            each(s, lambda c: c.start())
        for s in range(n):
            each(s, lambda c: c.wait())

    @pl.when(i < nf)
    def _():
        cols = pl.ds(pl.multiple_of(i * FT, FT), FT)

        def body(r, c):
            rows = pl.ds(pl.multiple_of(r * MT, MT), MT)
            xb = xs[rows, :]
            a = jnp.dot(xb, w1_ref[0], preferred_element_type=jnp.float32)
            b = jnp.dot(xb, w3_ref[0], preferred_element_type=jnp.float32)
            hs[rows, cols] = (jax.nn.silu(a) * b).astype(jnp.bfloat16)
            return c

        lax.fori_loop(0, tiles, body, 0)

    for j in range(nd):
        @pl.when(i == nf + j)
        def _():
            if j >= 2:
                for s in range(n):
                    put(s, j - 2).wait()

    @pl.when(i >= nf)
    def _():
        b = lax.rem(i - nf, 2)

        def body(r, c):
            rows = pl.ds(pl.multiple_of(r * MT, MT), MT)
            os[b, rows, :] = jnp.dot(hs[rows, :], w2_ref[0], preferred_element_type=jnp.float32).astype(os.dtype)
            return c

        lax.fori_loop(0, tiles, body, 0)

    for j in range(nd):
        @pl.when(i == nf + j)
        def _():
            for s in range(n):
                put(s, j).start()
            if j == nd - 1:
                for p in (nd - 2, nd - 1):
                    for s in range(n):
                        put(s, p).wait()


def _mlp(counts, srcs, w1, w3, w2, name):
    n = len(srcs)
    seg, d = srcs[0].shape
    ff = w1.shape[2]
    nf, nd = ff // FT, d // DT
    full = -(-n * seg // MT) * MT
    cap = -(-(n * seg + seg) // MT) * MT
    ends = jnp.cumsum((counts + (PIECE - 1)) // PIECE * PIECE)
    off = jnp.concatenate([jnp.zeros((1,), jnp.int32), ends.astype(jnp.int32)])
    any_spec = pl.BlockSpec(memory_space=pl.ANY)
    grid_spec = pltpu.PrefetchScalarGridSpec(
        num_scalar_prefetch=1,
        grid=(nf + nd,),
        in_specs=[any_spec] * n
        + [
            pl.BlockSpec((1, d, FT), lambda i, o: (0, 0, jnp.minimum(i, nf - 1))),
            pl.BlockSpec((1, d, FT), lambda i, o: (0, 0, jnp.minimum(i, nf - 1))),
            pl.BlockSpec((1, ff, DT), lambda i, o: (0, 0, jnp.maximum(i - nf, 0))),
        ],
        out_specs=[any_spec] * n,
        scratch_shapes=[
            pltpu.VMEM((cap, d), jnp.bfloat16),
            pltpu.VMEM((full, ff), jnp.bfloat16),
            pltpu.VMEM((2, cap, DT), jnp.bfloat16),
            pltpu.SemaphoreType.DMA((n, seg // PIECE)),
            pltpu.SemaphoreType.DMA((2, n)),
        ],
    )
    return pl.pallas_call(
        functools.partial(_mlp_kernel, nf, nd, n),
        grid_spec=grid_spec,
        out_shape=[jax.ShapeDtypeStruct((seg, d), jnp.bfloat16)] * n,
        compiler_params=_params(),
        cost_estimate=_cost(6 * n * seg * d * ff, 6 * d * ff),
        name=name,
    )(off, *srcs, w1, w3, w2)


def _combine_kernel(base, n, more, dest_ref, g_ref, *refs):
    srcs, refs = refs[:n], refs[n:]
    if more:
        acc_ref, refs = refs[0], refs[1:]
    o_ref, buf, sem = refs
    rows, (cap, _) = dest_ref.shape[0], buf.shape
    seg = cap // n

    @pl.when(pl.program_id(0) == 0)
    def _():
        copies = [pltpu.make_async_copy(srcs[s], buf.at[pl.ds(s * seg, seg), :], sem.at[s]) for s in range(n)]
        for c in copies:
            c.start()
        for c in copies:
            c.wait()

    r = lax.broadcasted_iota(jnp.int32, (rows, cap), 1) + base
    acc = acc_ref[...] if more else None
    for j in range(2):
        sel = (dest_ref[:, j : j + 1] == r).astype(jnp.bfloat16)
        op = g_ref[:, j : j + 1] * jnp.dot(sel, buf[...], preferred_element_type=jnp.float32)
        acc = op if acc is None else acc + op
    o_ref[...] = acc.astype(o_ref.dtype)


def _combine(dest, g, srcs, acc, base, last, name):
    t = dest.shape[0]
    n = len(srcs)
    seg, d = srcs[0].shape
    rows = 256
    more = acc is not None
    row = lambda i: (i, 0)
    return pl.pallas_call(
        functools.partial(_combine_kernel, base, n, more),
        grid=(t // rows,),
        in_specs=[pl.BlockSpec((rows, 2), row), pl.BlockSpec((rows, 2), row)]
        + [pl.BlockSpec(memory_space=pl.ANY)] * n
        + ([pl.BlockSpec((rows, d), row)] if more else []),
        out_specs=pl.BlockSpec((rows, d), row),
        out_shape=jax.ShapeDtypeStruct((t, d), jnp.bfloat16 if last else jnp.float32),
        scratch_shapes=[pltpu.VMEM((n * seg, d), jnp.bfloat16), pltpu.SemaphoreType.DMA((n,))],
        compiler_params=_params(),
        cost_estimate=_cost(4 * n * seg * t * d, 2 * d * (t + n * seg)),
        name=name,
    )(dest, g, *srcs, *([acc] if more else []))


def solution(mesh):
    n = mesh.shape['expert']
    perms = [[(i, i ^ s) for i in range(n)] for s in range(n)]

    def local(x, idx, wr, w1, w3, w2):
        t, d = x.shape
        k = idx.shape[1]
        cs = 2 * k * t // n
        me = lax.axis_index('expert')
        ids = jnp.arange(n, dtype=jnp.int32)

        it = idx.T
        oh = it[:, None, :] == ids[None, :, None]
        c = jnp.any(oh, axis=0)
        count = jnp.sum(c.astype(jnp.int32), axis=1)
        tok = jnp.arange(t, dtype=jnp.int32)
        tri = (tok[:, None] < tok[None, :]).astype(jnp.bfloat16)
        rank = jnp.dot(c.astype(jnp.bfloat16), tri, preferred_element_type=jnp.float32).astype(jnp.int32)
        rank = jnp.sum(jnp.where(oh, rank[None], 0), axis=1)
        rank = jnp.where(rank < cs, rank, 2 * cs)
        slot = jnp.bitwise_xor(it, me)
        logits = jnp.dot(x, wr, preferred_element_type=jnp.float32)
        g = jax.nn.softmax(jnp.sum(jnp.where(idx[:, :, None] == ids, logits[:, None, :], 0.0), axis=2), axis=-1)

        def swap(parts):
            return [parts[0]] + [lax.ppermute(parts[s], 'expert', perms[s]) for s in range(1, n)]

        def begin(segs):
            first, second = segs
            dest_t = jnp.where(
                rank < first,
                slot * first + rank,
                jnp.where(rank < first + second, n * first + slot * second + rank - first, -1),
            )
            sent = [_gather(x, dest_t, i * n * first, segs[i], n, f'gather{i}') for i in range(2)]
            return dest_t.T, swap(sent[0]), sent[1]

        def rest(segs, dest, got0, sent1, mine, g, w1, w3, w2):
            first, second = segs
            got0, sent1 = lax.optimization_barrier((got0, sent1))
            got1 = swap(sent1)
            res0 = _mlp(jnp.clip(mine, 0, first), got0, w1, w3, w2, 'mlp0')
            res0, got1 = lax.optimization_barrier((res0, got1))
            back0 = swap(res0)
            res1 = _mlp(jnp.clip(mine - first, 0, second), got1, w1, w3, w2, 'mlp1')
            back1 = swap(res1)
            h = n // 2
            acc = _combine(dest, g, back0, None, 0, False, 'combine0')
            acc = _combine(dest, g, back1[:h], acc, n * first, False, 'combine1')
            return _combine(dest, g, back1[h:], acc, n * first + h * second, True, 'combine2')

        dest, got0, sent1 = begin(FAST)
        count, got0[1] = lax.optimization_barrier((count, got0[1]))
        every = lax.all_gather(count, ('data', 'expert'))
        counts = jnp.minimum(lax.dynamic_slice_in_dim(every, lax.axis_index('data') * n, n), cs)
        mine = jnp.sum(jnp.where(ids[None, :] == me, counts, 0), axis=1)
        part = jnp.bitwise_xor(ids, me)
        mine = jnp.sum(jnp.where(part[:, None] == ids[None, :], mine[None, :], 0), axis=1)
        fits = jnp.minimum(jnp.max(every), cs) <= sum(FAST)
        y = rest(FAST, dest, got0, sent1, mine, g, w1, w3, w2)

        def full(y, mine, g, w1, w3, w2):
            segs = (cs // 2, cs // 2)
            return rest(segs, *begin(segs), mine, g, w1, w3, w2)

        return lax.cond(fits, lambda y, *_: y, full, y, mine, g, w1, w3, w2)

    tok = P(('data', 'expert'), None)
    wsp = P('expert', None, None)
    return jax.shard_map(local, mesh=mesh, in_specs=(tok, tok, P(), wsp, wsp, wsp), out_specs=tok, check_vma=False)
```

```python
import functools

import jax
import jax.numpy as jnp
from jax import lax
from jax.experimental import pallas as pl
from jax.experimental.pallas import tpu as pltpu
from jax.sharding import PartitionSpec as P

MT = 256
KEY = 4096
SLOW = 128
FT = 512
DT = 512
PIECE = 16
FAST = (128, 128, 112)
VMEM = 62 * 1024 * 1024


def _params():
    return pltpu.CompilerParams(vmem_limit_bytes=VMEM)


def _cost(flops, moved):
    return pl.CostEstimate(flops=flops, bytes_accessed=moved, transcendentals=0)


def _share_kernel(axis, n, c_ref, o_ref, send_sem, recv_sem):
    me = lax.axis_index(axis)
    peers = [{axis: lax.rem(me + k, n)} for k in range(n)]
    barrier = pltpu.get_barrier_semaphore()
    for k in range(1, n):
        pl.semaphore_signal(barrier, inc=1, device_id=peers[k], device_id_type=pl.DeviceIdType.MESH)
    own = pltpu.make_async_copy(c_ref, o_ref.at[me], send_sem.at[0])
    own.start()
    pl.semaphore_wait(barrier, n - 1)
    copies = [
        pltpu.make_async_remote_copy(
            src_ref=c_ref,
            dst_ref=o_ref.at[me],
            send_sem=send_sem.at[k],
            recv_sem=recv_sem.at[k],
            device_id=peers[k],
            device_id_type=pl.DeviceIdType.MESH,
        )
        for k in range(1, n)
    ]
    for c in copies:
        c.start()
    own.wait()
    for c in copies:
        c.wait()


def _share(c, axis, n, collective_id):
    return pl.pallas_call(
        functools.partial(_share_kernel, axis, n),
        in_specs=[pl.BlockSpec(memory_space=pltpu.VMEM)],
        out_specs=pl.BlockSpec(memory_space=pltpu.VMEM),
        out_shape=jax.ShapeDtypeStruct((n, 8, 128), jnp.int32),
        scratch_shapes=[pltpu.SemaphoreType.DMA((n,)), pltpu.SemaphoreType.DMA((n,))],
        compiler_params=pltpu.CompilerParams(collective_id=collective_id, has_side_effects=True),
        name=f'share_{axis}',
    )(c)


def _gather_kernel(slot, low, n, key_ref, x_ref, *refs):
    outs, buf, sem = refs[:n], refs[n], refs[n + 1]
    i = pl.program_id(0)
    rows, t = buf.shape[1], x_ref.shape[0]
    r = lax.broadcasted_iota(jnp.int32, (rows, t), 0) + ((slot + i) * KEY + low)
    hit = (r == key_ref[0:1, :]) | (r == key_ref[1:2, :])
    buf[i] = jnp.dot(hit.astype(jnp.bfloat16), x_ref[...], preferred_element_type=jnp.float32).astype(buf.dtype)
    for s in range(n):
        @pl.when(i == s)
        def _():
            pltpu.make_async_copy(buf.at[s], outs[s], sem.at[s]).start()

    @pl.when(i == n - 1)
    def _():
        for s in range(n):
            pltpu.make_async_copy(buf.at[s], outs[s], sem.at[s]).wait()


def _gather(x, key_t, slot, low, rows, n, name):
    t, d = x.shape
    return pl.pallas_call(
        functools.partial(_gather_kernel, slot, low, n),
        grid=(n,),
        in_specs=[
            pl.BlockSpec((2, t), lambda i: (0, 0)),
            pl.BlockSpec((t, d), lambda i: (0, 0), pipeline_mode=pl.Buffered(1)),
        ],
        out_specs=[pl.BlockSpec(memory_space=pl.ANY)] * n,
        out_shape=[jax.ShapeDtypeStruct((rows, d), x.dtype)] * n,
        scratch_shapes=[pltpu.VMEM((n, rows, d), x.dtype), pltpu.SemaphoreType.DMA((n,))],
        compiler_params=_params(),
        cost_estimate=_cost(2 * n * rows * t * d, 2 * d * (t + n * rows)),
        name=name,
    )(key_t, x)


def _mlp_kernel(nf, nd, n, halves, off_ref, *refs):
    srcs, (w1_ref, w3_ref, w2_ref), outs = refs[:n], refs[n : n + 3], refs[n + 3 : 2 * n + 3]
    xs, hs, os, in_sem, out_sem = refs[2 * n + 3 :]
    i = pl.program_id(0)
    seg = srcs[0].shape[0]
    total = off_ref[n]
    half = MT // 2
    tiles = (total + (half - 1 if halves else MT - 1)) // MT

    def over_rows(step):
        def body(r, c):
            step(pl.ds(pl.multiple_of(r * MT, MT), MT))
            return c

        lax.fori_loop(0, tiles, body, 0)
        if halves:
            @pl.when(total > tiles * MT)
            def _():
                step(pl.ds(pl.multiple_of(tiles * MT, MT), half))

    def place(s):
        return pl.ds(pl.multiple_of(off_ref[s], PIECE), seg)

    def put(s, j):
        return pltpu.make_async_copy(
            os.at[j % 2, place(s), :], outs[s].at[:, pl.ds(j * DT, DT)], out_sem.at[j % 2, s]
        )

    @pl.when(i == 0)
    def _():
        def clear(r, c):
            rows = pl.ds(pl.multiple_of(r * 128, 128), 128)
            xs[rows, :] = jnp.zeros((128, xs.shape[1]), xs.dtype)
            for b in range(2):
                os[b, rows, :] = jnp.zeros((128, DT), os.dtype)
            return c

        lax.fori_loop(0, xs.shape[0] // 128, clear, 0)

        def piece(s, p):
            at = pl.multiple_of(off_ref[s] + p * PIECE, PIECE)
            src = srcs[s].at[pl.ds(pl.multiple_of(p * PIECE, PIECE), PIECE), :]
            return pltpu.make_async_copy(src, xs.at[pl.ds(at, PIECE), :], in_sem.at[s, p])

        def each(s, act):
            def body(p, c):
                act(piece(s, p))
                return c

            lax.fori_loop(0, (off_ref[s + 1] - off_ref[s]) // PIECE, body, 0)

        for s in range(n):
            each(s, lambda c: c.start())
        for s in range(n):
            each(s, lambda c: c.wait())

    @pl.when(i < nf)
    def _():
        def step(rows):
            xb = xs[rows, :]
            a = jnp.dot(xb, w1_ref[0], preferred_element_type=jnp.float32)
            b = jnp.dot(xb, w3_ref[0], preferred_element_type=jnp.float32)
            hs[rows, pl.ds(pl.multiple_of(i * FT, FT), FT)] = (jax.nn.silu(a) * b).astype(jnp.bfloat16)

        over_rows(step)

    for j in range(nd):
        @pl.when(i == nf + j)
        def _():
            if j >= 2:
                for s in range(n):
                    put(s, j - 2).wait()

    @pl.when(i >= nf)
    def _():
        b = lax.rem(i - nf, 2)

        def step(rows):
            os[b, rows, :] = jnp.dot(hs[rows, :], w2_ref[0], preferred_element_type=jnp.float32).astype(os.dtype)

        over_rows(step)

    for j in range(nd):
        @pl.when(i == nf + j)
        def _():
            for s in range(n):
                put(s, j).start()
            if j == nd - 1:
                for p in (nd - 2, nd - 1):
                    for s in range(n):
                        put(s, p).wait()


def _mlp(counts, srcs, w1, w3, w2, name, halves=True):
    n = len(srcs)
    seg, d = srcs[0].shape
    ff = w1.shape[2]
    nf, nd = ff // FT, d // DT
    full = -(-n * seg // MT) * MT
    cap = -(-(n * seg + seg) // MT) * MT
    ends = jnp.cumsum((counts + (PIECE - 1)) // PIECE * PIECE)
    off = jnp.concatenate([jnp.zeros((1,), jnp.int32), ends.astype(jnp.int32)])
    any_spec = pl.BlockSpec(memory_space=pl.ANY)
    grid_spec = pltpu.PrefetchScalarGridSpec(
        num_scalar_prefetch=1,
        grid=(nf + nd,),
        in_specs=[any_spec] * n
        + [
            pl.BlockSpec((1, d, FT), lambda i, o: (0, 0, jnp.minimum(i, nf - 1))),
            pl.BlockSpec((1, d, FT), lambda i, o: (0, 0, jnp.minimum(i, nf - 1))),
            pl.BlockSpec((1, ff, DT), lambda i, o: (0, 0, jnp.maximum(i - nf, 0))),
        ],
        out_specs=[any_spec] * n,
        scratch_shapes=[
            pltpu.VMEM((cap, d), jnp.bfloat16),
            pltpu.VMEM((full, ff), jnp.bfloat16),
            pltpu.VMEM((2, cap, DT), jnp.bfloat16),
            pltpu.SemaphoreType.DMA((n, seg // PIECE)),
            pltpu.SemaphoreType.DMA((2, n)),
        ],
    )
    return pl.pallas_call(
        functools.partial(_mlp_kernel, nf, nd, n, halves),
        grid_spec=grid_spec,
        out_shape=[jax.ShapeDtypeStruct((seg, d), jnp.bfloat16)] * n,
        compiler_params=_params(),
        cost_estimate=_cost(6 * n * seg * d * ff, 6 * d * ff),
        name=name,
    )(off, *srcs, w1, w3, w2)


def _combine_kernel(blocks, more, key_ref, g_ref, *refs):
    n = len(blocks)
    srcs, refs = refs[:n], refs[n:]
    if more:
        acc_ref, refs = refs[0], refs[1:]
    o_ref, buf, sem = refs
    rows, (cap, _) = key_ref.shape[0], buf.shape
    starts = [sum(b[2] for b in blocks[:s]) for s in range(n)]

    @pl.when(pl.program_id(0) == 0)
    def _():
        copies = [
            pltpu.make_async_copy(srcs[s], buf.at[pl.ds(starts[s], blocks[s][2]), :], sem.at[s]) for s in range(n)
        ]
        for c in copies:
            c.start()
        for c in copies:
            c.wait()

    col = lax.broadcasted_iota(jnp.int32, (8, cap), 1)
    key, before = col, 0
    for (slot, low, _), start in zip(blocks, starts):
        shift = slot * KEY + low - start
        key = key + jnp.where(col >= start, shift - before, 0)
        before = shift
    key = key[0:1]
    acc = acc_ref[...] if more else None
    for j in range(2):
        sel = (key_ref[:, j : j + 1] == key).astype(jnp.bfloat16)
        op = g_ref[:, j : j + 1] * jnp.dot(sel, buf[...], preferred_element_type=jnp.float32)
        acc = op if acc is None else acc + op
    o_ref[...] = acc.astype(o_ref.dtype)


def _combine(keys, g, parts, acc, last, name):
    blocks = tuple((slot + i, low, src.shape[0]) for srcs, slot, low in parts for i, src in enumerate(srcs))
    srcs = [src for part in parts for src in part[0]]
    t, n, d = keys.shape[0], len(srcs), srcs[0].shape[1]
    cap = sum(b[2] for b in blocks)
    rows = 256
    more = acc is not None
    row = lambda i: (i, 0)
    return pl.pallas_call(
        functools.partial(_combine_kernel, blocks, more),
        grid=(t // rows,),
        in_specs=[pl.BlockSpec((rows, 2), row), pl.BlockSpec((rows, 2), row)]
        + [pl.BlockSpec(memory_space=pl.ANY)] * n
        + ([pl.BlockSpec((rows, d), row)] if more else []),
        out_specs=pl.BlockSpec((rows, d), row),
        out_shape=jax.ShapeDtypeStruct((t, d), jnp.bfloat16 if last else jnp.float32),
        scratch_shapes=[pltpu.VMEM((cap, d), jnp.bfloat16), pltpu.SemaphoreType.DMA((n,))],
        compiler_params=_params(),
        cost_estimate=_cost(4 * cap * t * d, 2 * d * (t + cap)),
        name=name,
    )(keys, g, *srcs, *([acc] if more else []))


def solution(mesh):
    n = mesh.shape['expert']
    perms = [[(i, i ^ s) for i in range(n)] for s in range(n)]

    def local(x, idx, wr, w1, w3, w2):
        t, d = x.shape
        k = idx.shape[1]
        cs = 2 * k * t // n
        me = lax.axis_index('expert')
        ids = jnp.arange(n, dtype=jnp.int32)

        it = idx.T
        oh = it[:, None, :] == ids[None, :, None]
        c = jnp.any(oh, axis=0)
        count = jnp.sum(c.astype(jnp.int32), axis=1)
        tok = jnp.arange(t, dtype=jnp.int32)
        tri = (tok[:, None] < tok[None, :]).astype(jnp.bfloat16)
        rank = jnp.dot(c.astype(jnp.bfloat16), tri, preferred_element_type=jnp.float32).astype(jnp.int32)
        rank = jnp.sum(jnp.where(oh, rank[None], 0), axis=1)
        key_t = jnp.where(rank < cs, jnp.bitwise_xor(it, me) * KEY + rank, -1)
        logits = jnp.dot(x, wr, preferred_element_type=jnp.float32)
        g = jax.nn.softmax(jnp.sum(jnp.where(idx[:, :, None] == ids, logits[:, None, :], 0.0), axis=2), axis=-1)

        h = n // 2

        def send(parts, first=0):
            return [p if s == 0 else lax.ppermute(p, 'expert', perms[s]) for s, p in enumerate(parts, first)]

        loads = jnp.zeros((8, 128), jnp.int32).at[0, :n].set(count)
        key_t, every = lax.optimization_barrier((key_t, _share(loads, 'expert', n, 0)))
        keys = key_t.T
        counts = jnp.minimum(every[:, 0, :n], cs)
        mine = jnp.sum(jnp.where(ids[None, :] == me, counts, 0), axis=1)
        part = jnp.bitwise_xor(ids, me)
        mine = jnp.sum(jnp.where(part[:, None] == ids[None, :], mine[None, :], 0), axis=1)

        segs, lows = FAST, (0, FAST[0], FAST[0] + FAST[1])
        top = h + 2
        far0 = send(_gather(x, key_t, h, 0, segs[0], 1, 'gather_lead'), h)
        far0 = far0 + send(_gather(x, key_t, h + 1, 0, segs[0], h - 1, 'gather_far'), h + 1)
        near0 = send(_gather(x, key_t, 0, 0, segs[0], h, 'gather_near'))
        sent1 = _gather(x, key_t, 0, lows[1], segs[1], n, 'gather1')
        lead1 = send(sent1[h : h + 1], h)
        sent2 = _gather(x, key_t, 0, lows[2], segs[2], n, 'gather2')

        every, near0[1] = lax.optimization_barrier((every, near0[1]))
        most = jnp.broadcast_to(jnp.max(every[:, 0, :n]), (8, 128))
        most = _share(most, 'data', mesh.shape['data'], 1)
        got0, sent1, sent2, most = lax.optimization_barrier((near0 + far0, sent1, sent2, most))
        fits = jnp.max(most) <= sum(FAST)
        used = [jnp.clip(mine - low, 0, seg) for low, seg in zip(lows, segs)]

        near1 = send(sent1[:h])
        far1 = lead1 + send(sent1[h + 1 :], h + 1)
        lead2 = send(sent2[h : h + 1], h)
        res0 = _mlp(used[0], got0, w1, w3, w2, 'mlp0')

        got1, res0, sent2 = lax.optimization_barrier((near1 + far1, res0, sent2))
        near2 = send(sent2[:h])
        far2 = lead2 + send(sent2[h + 1 :], h + 1)
        lead0 = send(res0[h:top], h)
        res1 = _mlp(used[1], got1, w1, w3, w2, 'mlp1')

        got2, res1, res0 = lax.optimization_barrier((near2 + far2, res1, res0))
        near0 = send(res0[:h])
        far0 = lead0 + send(res0[top:], top)
        lead1 = send(res1[h:top], h)
        res2 = _mlp(used[2], got2, w1, w3, w2, 'mlp2')

        res2, res1 = lax.optimization_barrier((res2, res1))
        near1 = send(res1[:h])
        far1 = lead1 + send(res1[top:], top)
        back0, res2 = lax.optimization_barrier((near0 + far0, res2))
        near2 = send(res2[:h])
        far2 = send(res2[h:], h)
        acc = _combine(keys, g, [(back0, 0, 0)], None, False, 'combine0')
        acc = _combine(keys, g, [(near1, 0, lows[1]), (far1[: top - h], h, lows[1])], acc, False, 'combine1')
        acc = _combine(keys, g, [(far1[top - h :], top, lows[1]), (near2, 0, lows[2])], acc, False, 'combine2')
        y = _combine(keys, g, [(far2, h, lows[2])], acc, True, 'combine3')

        def full(y, x, key_t, mine, g, w1, w3, w2):
            def chunk(i, acc):
                low = i * SLOW
                to = jnp.where(key_t >= 0, key_t - low, -1)
                to = jnp.where(key_t % KEY >= low, to, -1)
                got = send(_gather(x, to, 0, 0, SLOW, n, 'gather_full'))
                res = _mlp(jnp.clip(mine - low, 0, SLOW), got, w1, w3, w2, 'mlp_full', False)
                return _combine(to.T, g, [(send(res), 0, 0)], acc, False, 'combine_full')

            return lax.fori_loop(0, cs // SLOW, chunk, jnp.zeros((t, d), jnp.float32)).astype(x.dtype)

        return lax.cond(fits, lambda y, *_: y, full, y, x, key_t, mine, g, w1, w3, w2)

    tok = P(('data', 'expert'), None)
    wsp = P('expert', None, None)
    return jax.shard_map(local, mesh=mesh, in_specs=(tok, tok, P(), wsp, wsp, wsp), out_specs=tok, check_vma=False)
```

```python
import functools

import jax
import jax.numpy as jnp
from jax import lax
from jax.experimental import pallas as pl
from jax.experimental.pallas import tpu as pltpu
from jax.sharding import PartitionSpec as P

MT = 256
KEY = 4096
SLOW = 128
FT = 512
DT = 512
PIECE = 16
FAST = (128, 128, 112)
VMEM = 62 * 1024 * 1024


def _params():
    return pltpu.CompilerParams(vmem_limit_bytes=VMEM)


def _cost(flops, moved):
    return pl.CostEstimate(flops=flops, bytes_accessed=moved, transcendentals=0)


def _share_kernel(axis, n, c_ref, o_ref, send_sem, recv_sem):
    me = lax.axis_index(axis)
    peers = [{axis: lax.rem(me + k, n)} for k in range(n)]
    barrier = pltpu.get_barrier_semaphore()
    for k in range(1, n):
        pl.semaphore_signal(barrier, inc=1, device_id=peers[k], device_id_type=pl.DeviceIdType.MESH)
    own = pltpu.make_async_copy(c_ref, o_ref.at[me], send_sem.at[0])
    own.start()
    pl.semaphore_wait(barrier, n - 1)
    copies = [
        pltpu.make_async_remote_copy(
            src_ref=c_ref,
            dst_ref=o_ref.at[me],
            send_sem=send_sem.at[k],
            recv_sem=recv_sem.at[k],
            device_id=peers[k],
            device_id_type=pl.DeviceIdType.MESH,
        )
        for k in range(1, n)
    ]
    for c in copies:
        c.start()
    own.wait()
    for c in copies:
        c.wait()


def _share(c, axis, n, collective_id):
    return pl.pallas_call(
        functools.partial(_share_kernel, axis, n),
        in_specs=[pl.BlockSpec(memory_space=pltpu.VMEM)],
        out_specs=pl.BlockSpec(memory_space=pltpu.VMEM),
        out_shape=jax.ShapeDtypeStruct((n, 8, 128), jnp.int32),
        scratch_shapes=[pltpu.SemaphoreType.DMA((n,)), pltpu.SemaphoreType.DMA((n,))],
        compiler_params=pltpu.CompilerParams(collective_id=collective_id, has_side_effects=True),
        name=f'share_{axis}',
    )(c)


def _gather_kernel(slot, low, n, key_ref, x_ref, *refs):
    outs, buf, sem = refs[:n], refs[n], refs[n + 1]
    i = pl.program_id(0)
    rows, t = buf.shape[1], x_ref.shape[0]
    r = lax.broadcasted_iota(jnp.int32, (rows, t), 0) + ((slot + i) * KEY + low)
    hit = (r == key_ref[0:1, :]) | (r == key_ref[1:2, :])
    buf[i] = jnp.dot(hit.astype(jnp.bfloat16), x_ref[...], preferred_element_type=jnp.float32).astype(buf.dtype)
    for s in range(n):
        @pl.when(i == s)
        def _():
            pltpu.make_async_copy(buf.at[s], outs[s], sem.at[s]).start()

    @pl.when(i == n - 1)
    def _():
        for s in range(n):
            pltpu.make_async_copy(buf.at[s], outs[s], sem.at[s]).wait()


def _gather(x, key_t, slot, low, rows, n, name):
    t, d = x.shape
    return pl.pallas_call(
        functools.partial(_gather_kernel, slot, low, n),
        grid=(n,),
        in_specs=[
            pl.BlockSpec((2, t), lambda i: (0, 0)),
            pl.BlockSpec((t, d), lambda i: (0, 0), pipeline_mode=pl.Buffered(1)),
        ],
        out_specs=[pl.BlockSpec(memory_space=pl.ANY)] * n,
        out_shape=[jax.ShapeDtypeStruct((rows, d), x.dtype)] * n,
        scratch_shapes=[pltpu.VMEM((n, rows, d), x.dtype), pltpu.SemaphoreType.DMA((n,))],
        compiler_params=_params(),
        cost_estimate=_cost(2 * n * rows * t * d, 2 * d * (t + n * rows)),
        name=name,
    )(key_t, x)


def _mlp_kernel(nf, nd, n, halves, off_ref, *refs):
    srcs, (w1_ref, w3_ref, w2_ref), outs = refs[:n], refs[n : n + 3], refs[n + 3 : 2 * n + 3]
    xs, hs, os, in_sem, out_sem = refs[2 * n + 3 :]
    i = pl.program_id(0)
    seg = srcs[0].shape[0]
    total = off_ref[n]
    half = MT // 2
    tiles = (total + (half - 1 if halves else MT - 1)) // MT

    def over_rows(step):
        def body(r, c):
            step(pl.ds(pl.multiple_of(r * MT, MT), MT))
            return c

        lax.fori_loop(0, tiles, body, 0)
        if halves:
            @pl.when(total > tiles * MT)
            def _():
                step(pl.ds(pl.multiple_of(tiles * MT, MT), half))

    def place(s):
        return pl.ds(pl.multiple_of(off_ref[s], PIECE), seg)

    def put(s, j):
        return pltpu.make_async_copy(
            os.at[j % 2, place(s), :], outs[s].at[:, pl.ds(j * DT, DT)], out_sem.at[j % 2, s]
        )

    @pl.when(i == 0)
    def _():
        def clear(r, c):
            rows = pl.ds(pl.multiple_of(r * 128, 128), 128)
            xs[rows, :] = jnp.zeros((128, xs.shape[1]), xs.dtype)
            for b in range(2):
                os[b, rows, :] = jnp.zeros((128, DT), os.dtype)
            return c

        lax.fori_loop(0, xs.shape[0] // 128, clear, 0)

        def piece(s, p):
            at = pl.multiple_of(off_ref[s] + p * PIECE, PIECE)
            src = srcs[s].at[pl.ds(pl.multiple_of(p * PIECE, PIECE), PIECE), :]
            return pltpu.make_async_copy(src, xs.at[pl.ds(at, PIECE), :], in_sem.at[s, p])

        def each(s, act):
            def body(p, c):
                act(piece(s, p))
                return c

            lax.fori_loop(0, (off_ref[s + 1] - off_ref[s]) // PIECE, body, 0)

        for s in range(n):
            each(s, lambda c: c.start())
        for s in range(n):
            each(s, lambda c: c.wait())

    @pl.when(i < nf)
    def _():
        def step(rows):
            xb = xs[rows, :]
            a = jnp.dot(xb, w1_ref[0], preferred_element_type=jnp.float32)
            b = jnp.dot(xb, w3_ref[0], preferred_element_type=jnp.float32)
            hs[rows, pl.ds(pl.multiple_of(i * FT, FT), FT)] = (jax.nn.silu(a) * b).astype(jnp.bfloat16)

        over_rows(step)

    for j in range(nd):
        @pl.when(i == nf + j)
        def _():
            if j >= 2:
                for s in range(n):
                    put(s, j - 2).wait()

    @pl.when(i >= nf)
    def _():
        b = lax.rem(i - nf, 2)

        def step(rows):
            os[b, rows, :] = jnp.dot(hs[rows, :], w2_ref[0], preferred_element_type=jnp.float32).astype(os.dtype)

        over_rows(step)

    for j in range(nd):
        @pl.when(i == nf + j)
        def _():
            for s in range(n):
                put(s, j).start()
            if j == nd - 1:
                for p in (nd - 2, nd - 1):
                    for s in range(n):
                        put(s, p).wait()


def _mlp(counts, srcs, w1, w3, w2, name, halves=True):
    n = len(srcs)
    seg, d = srcs[0].shape
    ff = w1.shape[2]
    nf, nd = ff // FT, d // DT
    full = -(-n * seg // MT) * MT
    cap = -(-(n * seg + seg) // MT) * MT
    ends = jnp.cumsum((counts + (PIECE - 1)) // PIECE * PIECE)
    off = jnp.concatenate([jnp.zeros((1,), jnp.int32), ends.astype(jnp.int32)])
    any_spec = pl.BlockSpec(memory_space=pl.ANY)
    grid_spec = pltpu.PrefetchScalarGridSpec(
        num_scalar_prefetch=1,
        grid=(nf + nd,),
        in_specs=[any_spec] * n
        + [
            pl.BlockSpec((1, d, FT), lambda i, o: (0, 0, jnp.minimum(i, nf - 1))),
            pl.BlockSpec((1, d, FT), lambda i, o: (0, 0, jnp.minimum(i, nf - 1))),
            pl.BlockSpec((1, ff, DT), lambda i, o: (0, 0, jnp.maximum(i - nf, 0))),
        ],
        out_specs=[any_spec] * n,
        scratch_shapes=[
            pltpu.VMEM((cap, d), jnp.bfloat16),
            pltpu.VMEM((full, ff), jnp.bfloat16),
            pltpu.VMEM((2, cap, DT), jnp.bfloat16),
            pltpu.SemaphoreType.DMA((n, seg // PIECE)),
            pltpu.SemaphoreType.DMA((2, n)),
        ],
    )
    return pl.pallas_call(
        functools.partial(_mlp_kernel, nf, nd, n, halves),
        grid_spec=grid_spec,
        out_shape=[jax.ShapeDtypeStruct((seg, d), jnp.bfloat16)] * n,
        compiler_params=_params(),
        cost_estimate=_cost(6 * n * seg * d * ff, 6 * d * ff),
        name=name,
    )(off, *srcs, w1, w3, w2)


def _combine_kernel(blocks, more, key_ref, g_ref, *refs):
    n = len(blocks)
    srcs, refs = refs[:n], refs[n:]
    if more:
        acc_ref, refs = refs[0], refs[1:]
    o_ref, buf, sem = refs
    rows, (cap, _) = key_ref.shape[0], buf.shape
    starts = [sum(b[2] for b in blocks[:s]) for s in range(n)]

    @pl.when(pl.program_id(0) == 0)
    def _():
        copies = [
            pltpu.make_async_copy(srcs[s], buf.at[pl.ds(starts[s], blocks[s][2]), :], sem.at[s]) for s in range(n)
        ]
        for c in copies:
            c.start()
        for c in copies:
            c.wait()

    col = lax.broadcasted_iota(jnp.int32, (8, cap), 1)
    key, before = col, 0
    for (slot, low, _), start in zip(blocks, starts):
        shift = slot * KEY + low - start
        key = key + jnp.where(col >= start, shift - before, 0)
        before = shift
    key = key[0:1]
    acc = acc_ref[...] if more else None
    for j in range(2):
        sel = (key_ref[:, j : j + 1] == key).astype(jnp.bfloat16)
        op = g_ref[:, j : j + 1] * jnp.dot(sel, buf[...], preferred_element_type=jnp.float32)
        acc = op if acc is None else acc + op
    o_ref[...] = acc.astype(o_ref.dtype)


def _combine(keys, g, parts, acc, last, name):
    blocks = tuple((slot + i, low, src.shape[0]) for srcs, slot, low in parts for i, src in enumerate(srcs))
    srcs = [src for part in parts for src in part[0]]
    t, n, d = keys.shape[0], len(srcs), srcs[0].shape[1]
    cap = sum(b[2] for b in blocks)
    rows = 256
    more = acc is not None
    row = lambda i: (i, 0)
    return pl.pallas_call(
        functools.partial(_combine_kernel, blocks, more),
        grid=(t // rows,),
        in_specs=[pl.BlockSpec((rows, 2), row), pl.BlockSpec((rows, 2), row)]
        + [pl.BlockSpec(memory_space=pl.ANY)] * n
        + ([pl.BlockSpec((rows, d), row)] if more else []),
        out_specs=pl.BlockSpec((rows, d), row),
        out_shape=jax.ShapeDtypeStruct((t, d), jnp.bfloat16 if last else jnp.float32),
        scratch_shapes=[pltpu.VMEM((cap, d), jnp.bfloat16), pltpu.SemaphoreType.DMA((n,))],
        compiler_params=_params(),
        cost_estimate=_cost(4 * cap * t * d, 2 * d * (t + cap)),
        name=name,
    )(keys, g, *srcs, *([acc] if more else []))


def solution(mesh):
    n = mesh.shape['expert']
    perms = [[(i, i ^ s) for i in range(n)] for s in range(n)]

    def local(x, idx, wr, w1, w3, w2):
        t, d = x.shape
        k = idx.shape[1]
        cs = 2 * k * t // n
        me = lax.axis_index('expert')
        ids = jnp.arange(n, dtype=jnp.int32)

        it = idx.T
        oh = it[:, None, :] == ids[None, :, None]
        c = jnp.any(oh, axis=0)
        count = jnp.sum(c.astype(jnp.int32), axis=1)
        tok = jnp.arange(t, dtype=jnp.int32)
        tri = (tok[:, None] < tok[None, :]).astype(jnp.bfloat16)
        rank = jnp.dot(c.astype(jnp.bfloat16), tri, preferred_element_type=jnp.float32).astype(jnp.int32)
        rank = jnp.sum(jnp.where(oh, rank[None], 0), axis=1)
        key_t = jnp.where(rank < cs, jnp.bitwise_xor(it, me) * KEY + rank, -1)
        logits = jnp.dot(x, wr, preferred_element_type=jnp.float32)
        g = jax.nn.softmax(jnp.sum(jnp.where(idx[:, :, None] == ids, logits[:, None, :], 0.0), axis=2), axis=-1)

        h = n // 2

        def send(parts, first=0):
            return [p if s == 0 else lax.ppermute(p, 'expert', perms[s]) for s, p in enumerate(parts, first)]

        first = _gather(x, key_t, h, 0, FAST[0], 1, 'gather_lead')
        loads = jnp.zeros((8, 128), jnp.int32).at[0, :n].set(count)
        first, loads = lax.optimization_barrier((first, loads))
        lead = send(first, h)
        key_t, every = lax.optimization_barrier((key_t, _share(loads, 'expert', n, 0)))
        keys = key_t.T
        counts = jnp.minimum(every[:, 0, :n], cs)
        mine = jnp.sum(jnp.where(ids[None, :] == me, counts, 0), axis=1)
        part = jnp.bitwise_xor(ids, me)
        mine = jnp.sum(jnp.where(part[:, None] == ids[None, :], mine[None, :], 0), axis=1)

        segs, lows = FAST, (0, FAST[0], FAST[0] + FAST[1])
        top = h + 2
        far0 = lead + send(_gather(x, key_t, h + 1, 0, segs[0], h - 1, 'gather_far'), h + 1)
        near0 = send(_gather(x, key_t, 0, 0, segs[0], h, 'gather_near'))
        sent1 = _gather(x, key_t, 0, lows[1], segs[1], n, 'gather1')
        lead1 = send(sent1[h : h + 1], h)
        sent2 = _gather(x, key_t, 0, lows[2], segs[2], n, 'gather2')

        every, near0[1] = lax.optimization_barrier((every, near0[1]))
        most = jnp.broadcast_to(jnp.max(every[:, 0, :n]), (8, 128))
        most = _share(most, 'data', mesh.shape['data'], 1)
        got0, sent1, sent2, most = lax.optimization_barrier((near0 + far0, sent1, sent2, most))
        fits = jnp.max(most) <= sum(FAST)
        used = [jnp.clip(mine - low, 0, seg) for low, seg in zip(lows, segs)]

        near1 = send(sent1[:h])
        far1 = lead1 + send(sent1[h + 1 :], h + 1)
        lead2 = send(sent2[h : h + 1], h)
        res0 = _mlp(used[0], got0, w1, w3, w2, 'mlp0')

        got1, res0, sent2 = lax.optimization_barrier((near1 + far1, res0, sent2))
        near2 = send(sent2[:h])
        far2 = lead2 + send(sent2[h + 1 :], h + 1)
        lead0 = send(res0[h:top], h)
        res1 = _mlp(used[1], got1, w1, w3, w2, 'mlp1')

        got2, res1, res0 = lax.optimization_barrier((near2 + far2, res1, res0))
        near0 = send(res0[:h])
        far0 = lead0 + send(res0[top:], top)
        lead1 = send(res1[h:top], h)
        res2 = _mlp(used[2], got2, w1, w3, w2, 'mlp2')

        res2, res1 = lax.optimization_barrier((res2, res1))
        near1 = send(res1[:h])
        far1 = lead1 + send(res1[top:], top)
        back0, res2 = lax.optimization_barrier((near0 + far0, res2))
        near2 = send(res2[:h])
        far2 = send(res2[h:], h)
        acc = _combine(keys, g, [(back0, 0, 0)], None, False, 'combine0')
        acc = _combine(keys, g, [(near1, 0, lows[1]), (far1[: top - h], h, lows[1])], acc, False, 'combine1')
        acc = _combine(keys, g, [(far1[top - h :], top, lows[1]), (near2, 0, lows[2])], acc, False, 'combine2')
        y = _combine(keys, g, [(far2, h, lows[2])], acc, True, 'combine3')

        def full(y, x, key_t, mine, g, w1, w3, w2):
            def chunk(i, acc):
                low = i * SLOW
                to = jnp.where(key_t >= 0, key_t - low, -1)
                to = jnp.where(key_t % KEY >= low, to, -1)
                got = send(_gather(x, to, 0, 0, SLOW, n, 'gather_full'))
                res = _mlp(jnp.clip(mine - low, 0, SLOW), got, w1, w3, w2, 'mlp_full', False)
                return _combine(to.T, g, [(send(res), 0, 0)], acc, False, 'combine_full')

            return lax.fori_loop(0, cs // SLOW, chunk, jnp.zeros((t, d), jnp.float32)).astype(x.dtype)

        return lax.cond(fits, lambda y, *_: y, full, y, x, key_t, mine, g, w1, w3, w2)

    tok = P(('data', 'expert'), None)
    wsp = P('expert', None, None)
    return jax.shard_map(local, mesh=mesh, in_specs=(tok, tok, P(), wsp, wsp, wsp), out_specs=tok, check_vma=False)
```
